32 devices in a mesh: gx: 4 (over x, core), gy: 8 (over z, y).
Axes of the slice: x: 2, y: 2, z: 4, core: 2. Of those that a mesh axis runs over, the one named last changes fastest.
Arguments:
- mask_feats: bfloat16 [64, 8, 14, 14, 256], P(('gx', 'gy')), may hold values from -6 to 6
- mask_cot: bfloat16 [64, 8, 14, 14, 256], P(('gx', 'gy')), may hold values from -6 to 6
- roi_counts: int32 [64], P(('gx', 'gy')), may hold values from 1 to 8, as said below
- rpn_feats: bfloat16 [64, 48, 32, 256], P(('gx', 'gy')), may hold values from -6 to 6
- rpn_cot: bfloat16 [64, 48, 32, 256], P(('gx', 'gy')), may hold values from -360 to 360
- anchor_counts: int32 [64], P(('gx', 'gy')), may hold values from 32 to 223
- mask_weight: float32 [2304, 256], replicated, may hold values from -0.125 to 0.125
- rpn_weight: float32 [2304, 256], replicated, may hold values from -0.125 to 0.125
- mask_moment: float32 [2304, 256], replicated, may hold values from -6 to 6
- rpn_moment: float32 [2304, 256], replicated, may hold values from -6 to 6
Outputs:
- new_mask_weight: float32 [2304, 256], replicated
- new_rpn_weight: float32 [2304, 256], replicated
- new_mask_moment: float32 [2304, 256], replicated
- new_rpn_moment: float32 [2304, 256], replicated
The draws below stay inside these ranges and needn't reach their ends.
Inputs may be any that keep to these rules, and one draw needn't show every extreme that they name: `roi_counts`: every image has at least one positive ROI; some image has all 8 slots positive.
All inputs are finite; a program needn't handle non-finite values.
Results may differ from the reference program's by a relative error of at most 0.0003.
Values sent between devices are 32-bit elements; how exact they have to be, the bound alone decides.
A program may use at most 128 MiB of HBM per device.

```python
import jax
import jax.numpy as jnp
from jax import lax

C = 256
MH = 14
ROI_IMG = 8
IMG_DEV = 2
GH = 48
GW = 32
IMAGES = 64
N_GX = 4
N_GY = 8


def rising_level():
    image = jnp.arange(IMAGES, dtype=jnp.int32)
    device = image // IMG_DEV
    x_index = device // N_GY
    y_index = device % N_GY
    x_span = max(N_GX - 1, 1)
    y_span = max(N_GY - 1, 1)
    numer = x_index * y_span + y_index * x_span
    denom = 2 * x_span * y_span
    return (image, numer, denom)


def draw_roi_counts(key, part):
    image, numer, denom = rising_level()
    lowest = 1 + ROI_IMG * 5 // 8 * numer // denom
    extra = jax.random.randint(jax.random.fold_in(key, 11), (IMAGES,), 0, 3)
    counts = jnp.minimum(lowest + extra, ROI_IMG)
    counts = jnp.where(image == IMAGES - 1, ROI_IMG, counts)
    return counts.astype(jnp.int32)


def draw_anchor_counts(key, part):
    image, numer, denom = rising_level()
    lowest = 32 + 96 * numer // denom
    extra = jax.random.randint(jax.random.fold_in(key, 23), (IMAGES,), 0, 96)
    return (lowest + extra).astype(jnp.int32)


def level_of(own_key, shape, cuts, least, largest):
    gain = 1.0
    for axis_at, shards_of in cuts:
        draws = jax.random.uniform(jax.random.fold_in(jax.random.fold_in(own_key, 6), axis_at), (shards_of,), jnp.float32, least / len(cuts), largest / len(cuts))
        gain = gain * jnp.repeat(jnp.exp(draws), shape[axis_at] // shards_of).reshape((-1,) + (1,) * (len(shape) - 1 - axis_at))
    return gain


def bell_draw(key, shape, spread, limit, pieces=(), held_as=jnp.bfloat16):
    loudness = level_of(key, shape, pieces, -0.22, 0.18) if pieces else 1.0
    result = jax.random.normal(key, shape, jnp.float32) * spread * loudness
    return jnp.minimum(jnp.maximum(result, -limit), limit).astype(held_as)


def setup_inputs(seed: int = 0) -> dict:
    key_list = jax.random.split(jax.random.key(seed), 11)
    return {
        "mask_feats": bell_draw(key_list[0], (IMAGES, ROI_IMG, MH, MH, C), 1.0, 6.0, ((0, 32),)),
        "mask_cot": bell_draw(key_list[1], (IMAGES, ROI_IMG, MH, MH, C), 1.0, 6.0, ((0, 32),)),
        "roi_counts": draw_roi_counts(jax.random.fold_in(key_list[10], 71), 0),
        "rpn_feats": bell_draw(key_list[3], (IMAGES, GH, GW, C), 1.0, 6.0, ((0, 32),)),
        "rpn_cot": bell_draw(key_list[4], (IMAGES, GH, GW, C), 60.0, 360.0, ((0, 32),)),
        "anchor_counts": draw_anchor_counts(jax.random.fold_in(key_list[10], 71), 0),
        "mask_weight": bell_draw(key_list[6], (9 * C, C), (9 * C) ** -0.5, 0.125, (), jnp.float32),
        "rpn_weight": bell_draw(key_list[7], (9 * C, C), (9 * C) ** -0.5, 0.125, (), jnp.float32),
        "mask_moment": bell_draw(key_list[8], (9 * C, C), 1.0, 6.0, (), jnp.float32),
        "rpn_moment": bell_draw(key_list[9], (9 * C, C), 1.0, 6.0, (), jnp.float32),
    }


def weight_grad(feats, cotan):
    grid_rows = feats.shape[1]
    grid_cols = feats.shape[2]
    chans = feats.shape[3]
    padded = jnp.pad(feats, ((0, 0), (1, 1), (1, 1), (0, 0)))
    flat_cot = cotan.reshape(-1, chans)
    blocks = []
    for row_tap in range(3):
        for col_tap in range(3):
            window = padded[:, row_tap:row_tap + grid_rows, col_tap:col_tap + grid_cols, :].reshape(-1, chans)
            blocks.append(lax.dot_general(window, flat_cot, (((0,), (0,)), ((), ())), preferred_element_type=jnp.float32))
    return jnp.concatenate(blocks, axis=0)

def reference(mask_feats, mask_cot, roi_counts, rpn_feats, rpn_cot, anchor_counts, mask_weight, rpn_weight, mask_moment, rpn_moment):
    roi_total = jnp.sum(roi_counts).astype(jnp.float32)
    anchor_total = jnp.sum(anchor_counts).astype(jnp.float32)
    slots = jnp.arange(ROI_IMG, dtype=jnp.int32)
    valid_slots = (slots[None, :] < roi_counts[:, None]).astype(jnp.bfloat16)
    masked = mask_cot * valid_slots[:, :, None, None, None]
    mask_grad = weight_grad(mask_feats.reshape(-1, MH, MH, C), masked.reshape(-1, MH, MH, C)) / roi_total
    rpn_grad = weight_grad(rpn_feats, rpn_cot) / anchor_total
    new_mask_moment = 0.9 * mask_moment + mask_grad
    new_rpn_moment = 0.9 * rpn_moment + rpn_grad
    new_mask_weight = mask_weight - 0.02 * new_mask_moment
    new_rpn_weight = rpn_weight - 0.02 * new_rpn_moment
    return (new_mask_weight, new_rpn_weight, new_mask_moment, new_rpn_moment)
```

```python
import functools

import jax
import jax.numpy as jnp
from jax import lax
from jax.experimental import pallas as pl
from jax.experimental.pallas import tpu as pltpu
from jax.sharding import PartitionSpec as P

MESH = pl.DeviceIdType.MESH
TAPS = 9
LAG = 2


def dot_t(lhs, rhs):
    return lax.dot_general(lhs, rhs, (((0,), (0,)), ((), ())), preferred_element_type=jnp.float32)


def grads_kernel(counts, mask_x, mask_y, rpn_x, rpn_y, mask_g, rpn_g, xs, tmp, ycat_m, ycat_r):
    images, slots, side, _, chans = mask_x.shape
    cols = xs.shape[2]
    roi_rows = cols * cols
    xs[...] = jnp.zeros_like(xs)
    tmp[...] = jnp.zeros_like(tmp)
    ycat_m[...] = jnp.zeros_like(ycat_m)

    def one_roi(i, carry):
        n, s = lax.div(i, slots), lax.rem(i, slots)
        valid = s < counts[n]
        for y in range(side):
            xs[i, y, pl.ds(0, side), :] = mask_x[n, s, y]
            row = mask_y[n, s, y].astype(jnp.float32)
            tmp[y, pl.ds(0, side), :] = jnp.where(valid, row, 0.0)
        v = tmp[...].reshape(side * cols, chans)
        at = pl.ds(pl.multiple_of(cols + i * roi_rows, cols), side * cols)
        ycat_m[at, 0:chans] = pltpu.roll(v, side * cols - 1, 0).astype(jnp.bfloat16)
        ycat_m[at, chans : 2 * chans] = v.astype(jnp.bfloat16)
        ycat_m[at, 2 * chans :] = pltpu.roll(v, 1, 0).astype(jnp.bfloat16)
        return carry

    lax.fori_loop(0, images * slots, one_roi, 0)
    mask_g[...] = jnp.zeros_like(mask_g)
    per = 4
    block = per * roi_rows

    def mask_step(k, carry):
        x = xs[pl.ds(k * per, per)].reshape(block, chans)
        for a in range(3):
            base = pl.multiple_of(k * block + cols - (a - 1) * cols, cols)
            out = dot_t(x, ycat_m[pl.ds(base, block), :])
            for b in range(3):
                mask_g[3 * a + b] += out[:, b * chans : (b + 1) * chans]
        return carry

    lax.fori_loop(0, images * slots // per, mask_step, 0)

    _, grid_rows, grid_cols, _ = rpn_x.shape
    group = 8
    part = group * grid_cols
    rpn_g[...] = jnp.zeros_like(rpn_g)
    where_col = lax.rem(lax.broadcasted_iota(jnp.int32, (part, chans), 0), grid_cols)
    zero_rows = jnp.zeros((grid_cols, 3 * chans), jnp.bfloat16)
    ycat_r[pl.ds(0, grid_cols), :] = zero_rows
    ycat_r[pl.ds((1 + grid_rows) * grid_cols, grid_cols), :] = zero_rows

    def one_image(n, carry):
        def shift(r, inner):
            v = rpn_y[n, pl.ds(r * group, group)].reshape(part, chans)
            wide = v.astype(jnp.float32)
            down = jnp.where(where_col == grid_cols - 1, 0.0, pltpu.roll(wide, part - 1, 0))
            up = jnp.where(where_col == 0, 0.0, pltpu.roll(wide, 1, 0))
            at = pl.ds(pl.multiple_of(grid_cols + r * part, grid_cols), part)
            ycat_r[at, 0:chans] = down.astype(jnp.bfloat16)
            ycat_r[at, chans : 2 * chans] = v
            ycat_r[at, 2 * chans :] = up.astype(jnp.bfloat16)
            return inner

        lax.fori_loop(0, grid_rows // group, shift, 0)
        block_rows = 24
        depth = block_rows * grid_cols

        def rpn_step(k, inner):
            x = rpn_x[n, pl.ds(k * block_rows, block_rows)].reshape(depth, chans)
            for a in range(3):
                base = pl.multiple_of(k * depth + grid_cols - (a - 1) * grid_cols, grid_cols)
                out = dot_t(x, ycat_r[pl.ds(base, depth), :])
                for b in range(3):
                    rpn_g[3 * a + b] += out[:, b * chans : (b + 1) * chans]
            return inner

        lax.fori_loop(0, grid_rows // block_rows, rpn_step, 0)
        return carry

    lax.fori_loop(0, images, one_image, 0)


def local_grads(roi_counts, mask_feats, mask_cot, rpn_feats, rpn_cot):
    images, slots, side, _, chans = mask_feats.shape
    _, grid_rows, grid_cols, _ = rpn_feats.shape
    cols = -(-(side + 1) // 16) * 16
    vmem = pl.BlockSpec(memory_space=pltpu.VMEM)
    rows_m = images * slots * cols * cols
    out = jax.ShapeDtypeStruct((TAPS, chans, chans), jnp.float32)
    return pl.pallas_call(
        grads_kernel,
        out_shape=(out, out),
        in_specs=[pl.BlockSpec(memory_space=pltpu.SMEM)] + [vmem] * 4,
        out_specs=(vmem, vmem),
        scratch_shapes=[
            pltpu.VMEM((images * slots, cols, cols, chans), jnp.bfloat16),
            pltpu.VMEM((side, cols, chans), jnp.float32),
            pltpu.VMEM((rows_m + 2 * cols, 3 * chans), jnp.bfloat16),
            pltpu.VMEM(((grid_rows + 2) * grid_cols, 3 * chans), jnp.bfloat16),
        ],
        compiler_params=pltpu.CompilerParams(vmem_limit_bytes=56 * 2**20),
        name="grads",
    )(roi_counts, mask_feats, mask_cot, rpn_feats, rpn_cot)


def splits(rows, size):
    return rows % (8 * size) == 0


def groups_here(n_gx, n_gy):
    gx, gy = lax.axis_index("gx"), lax.axis_index("gy")
    core, x = lax.rem(gx, 2), lax.div(gx, 2)
    y, z = lax.rem(gy, 2), lax.div(gy, 2)
    core_group = (2, core, lambda m: (x * 2 + m, gy))
    x_group = (n_gx // 2, x, lambda m: (m * 2 + core, gy))
    y_group = (2, y, lambda m: (gx, z * 2 + m))
    z_group = (n_gy // 2, z, lambda m: (gx, m * 2 + y))
    return core_group, x_group, y_group, z_group


def members(group):
    size, own, device = group
    return [
        (k, lax.rem(own + 1 + k, size), size - 2 - k, device) for k in range(size - 1)
    ]


def sum_kernel(n_gx, n_gy, *refs):
    roi, anchor, mask_g, rpn_g, mask_mo, rpn_mo, mask_out, rpn_out = refs[:8]
    acc, mine, mine_sem, cnt, cnt_in = refs[8:13]
    landing = (refs[13:17], refs[17:21])
    cnt_sems = refs[21:25]
    cnt_send = refs[25:29]
    rs_recv = (refs[29:33], refs[33:37])
    rs_send = (refs[37:41], refs[41:45])
    ag_recv = (refs[45:49], refs[49:53])
    ag_send = (refs[53:57], refs[57:61])
    core_g, x_g, y_g, z_g = groups_here(n_gx, n_gy)
    orders = ((core_g, x_g, y_g, z_g), (core_g, y_g, x_g, z_g))
    grads, outs, moments = (mask_g, rpn_g), (mask_out, rpn_out), (mask_mo, rpn_mo)
    chunk = mask_g.shape[1]
    chunks = mask_g.shape[0]

    blocks, offs = [], []
    cut = ([], [])
    for color in range(2):
        b, o, bs, os = chunk, 0, [], [0]
        rest = chunk
        for size, _, _ in orders[color]:
            cut[color].append(splits(rest, size))
            rest = rest // size if cut[color][-1] else rest
        for size, own, _ in orders[color]:
            if splits(b, size):
                b = b // size
                o = o + own * b
            bs.append(b)
            os.append(o)
        blocks.append(bs)
        offs.append(os)
    piece = blocks[0][3]

    barrier = pltpu.get_barrier_semaphore()
    total = 0
    for g in orders[0]:
        for _, m, _, device in members(g):
            pl.semaphore_signal(barrier, inc=1, device_id=device(m), device_id_type=MESH)
            total += 1

    def own_rows(color, j):
        return pltpu.make_async_copy(
            moments[color].at[j, pl.ds(pl.multiple_of(offs[color][4], 8), piece), :],
            mine.at[color, j],
            mine_sem.at[color, j],
        )

    def start_moments(j, carry):
        own_rows(0, j).start()
        own_rows(1, j).start()
        return carry

    lax.fori_loop(0, chunks, start_moments, 0)
    half = cnt.shape[1] // 2
    lanes = cnt.shape[2]
    for which, ref in ((0, roi), (1, anchor)):
        s = ref[0]
        for i in range(1, ref.shape[0]):
            s = s + ref[i]
        cnt[0, which * half : (which + 1) * half, :] = jnp.full(
            (half, lanes), s.astype(jnp.float32), jnp.float32
        )
    pl.semaphore_wait(barrier, total)

    def cnt_copy(s, k, m, far, device):
        return pltpu.make_async_remote_copy(
            src_ref=cnt.at[s],
            dst_ref=cnt_in.at[s, far],
            send_sem=cnt_send[s].at[k],
            recv_sem=cnt_sems[s].at[far],
            device_id=device(m),
            device_id_type=MESH,
        )

    def cnt_arrival(s, k, m, device):
        return pltpu.make_async_remote_copy(
            src_ref=cnt.at[s],
            dst_ref=cnt_in.at[s, k],
            send_sem=cnt_send[s].at[k],
            recv_sem=cnt_sems[s].at[k],
            device_id=device(m),
            device_id_type=MESH,
        )

    def cnt_start(s):
        for k, m, far, device in members(orders[0][s]):
            cnt_copy(s, k, m, far, device).start()

    def cnt_finish(s):
        value = cnt[s]
        for k, m, far, device in members(orders[0][s]):
            cnt_arrival(s, k, m, device).wait_recv()
            value = value + cnt_in[s, k]
        cnt[s + 1] = value

    def rs_copy(color, s, j, k, m, far, device):
        b = blocks[color][s]
        start = offs[color][s] + (m * b if cut[color][s] else 0)
        rows = pl.ds(pl.multiple_of(start, 8), b)
        source = grads[color].at[j, rows, :] if s == 0 else acc.at[color, j, rows, :]
        return pltpu.make_async_remote_copy(
            src_ref=source,
            dst_ref=landing[color][s].at[j, far],
            send_sem=rs_send[color][s].at[j, k],
            recv_sem=rs_recv[color][s].at[j, far],
            device_id=device(m),
            device_id_type=MESH,
        )

    def rs_arrival(color, s, j, k, m, device):
        b = blocks[color][s]
        start = offs[color][s] + (m * b if cut[color][s] else 0)
        rows = pl.ds(pl.multiple_of(start, 8), b)
        source = grads[color].at[j, rows, :] if s == 0 else acc.at[color, j, rows, :]
        return pltpu.make_async_remote_copy(
            src_ref=source,
            dst_ref=landing[color][s].at[j, k],
            send_sem=rs_send[color][s].at[j, k],
            recv_sem=rs_recv[color][s].at[j, k],
            device_id=device(m),
            device_id_type=MESH,
        )

    def rs_start(color, s, j):
        for k, m, far, device in members(orders[color][s]):
            rs_copy(color, s, j, k, m, far, device).start()

    def rs_sum(color, s, j):
        b = blocks[color][s]
        rows = pl.ds(pl.multiple_of(offs[color][s + 1], 8), b)
        value = grads[color][j, rows, :] if s == 0 else acc[color, j, rows, :]
        for k, m, _, device in members(orders[color][s]):
            rs_arrival(color, s, j, k, m, device).wait_recv()
            if cut[color][s]:
                value = value + landing[color][s][j, k]
        if not cut[color][s]:
            size, own, _ = orders[color][s]
            terms = []
            for m in range(size):
                slot = lax.rem(m - own - 1 + 2 * size, size)
                slot = jnp.minimum(slot, max(size - 2, 0))
                here = own == m
                terms.append(jnp.where(here, value, landing[color][s][j, slot]))
            value = functools.reduce(jnp.add, terms) if size > 1 else value
        if s < 3:
            acc[color, j, rows, :] = value
        else:
            own_rows(color, j).wait()
            count = cnt[4, color * half : (color + 1) * half, :][0:1, :]
            count = jnp.concatenate([count] * (value.shape[1] // lanes), axis=1)
            outs[color][j, rows, :] = 0.9 * mine[color, j] + value / count

    def ag_copy(color, s, j, k, m, far, device):
        b = blocks[color][s]
        rows = pl.ds(pl.multiple_of(offs[color][s + 1], 8), b)
        return pltpu.make_async_remote_copy(
            src_ref=outs[color].at[j, rows, :],
            dst_ref=outs[color].at[j, rows, :],
            send_sem=ag_send[color][s].at[j, k],
            recv_sem=ag_recv[color][s].at[j, far],
            device_id=device(m),
            device_id_type=MESH,
        )

    def ag_arrival(color, s, j, k, m, device):
        b = blocks[color][s]
        rows = pl.ds(pl.multiple_of(offs[color][s] + m * b, 8), b)
        return pltpu.make_async_remote_copy(
            src_ref=outs[color].at[j, rows, :],
            dst_ref=outs[color].at[j, rows, :],
            send_sem=ag_send[color][s].at[j, k],
            recv_sem=ag_recv[color][s].at[j, k],
            device_id=device(m),
            device_id_type=MESH,
        )

    def ag_start(color, s, j):
        if not cut[color][s]:
            return
        for k, m, far, device in members(orders[color][s]):
            ag_copy(color, s, j, k, m, far, device).start()

    def ag_wait(color, s, j):
        if not cut[color][s]:
            return
        for k, m, _, device in members(orders[color][s]):
            ag_arrival(color, s, j, k, m, device).wait_recv()

    def at_stage(t, lag, work):
        j = t - lag

        @pl.when((j >= 0) & (j < chunks))
        def _():
            work(j)

    def tick(t, carry):
        def first(j):
            for color in range(2):
                rs_start(color, 0, j)

        at_stage(t, 0, first)
        for s in range(4):

            @pl.when(t == LAG * (s + 1))
            def _(s=s):
                cnt_finish(s)
                if s < 3:
                    cnt_start(s + 1)

        for s in range(4):

            def reduce(j, s=s):
                for color in range(2):
                    rs_sum(color, s, j)
                for color in range(2):
                    if s < 3:
                        rs_start(color, s + 1, j)
                    else:
                        ag_start(color, 3, j)

            at_stage(t, LAG * (s + 1), reduce)
        for s in (3, 2, 1, 0):

            def gather(j, s=s):
                for color in range(2):
                    ag_wait(color, s, j)
                    if s > 0:
                        ag_start(color, s - 1, j)

            at_stage(t, LAG * (8 - s), gather)
        return carry

    cnt_start(0)
    lax.fori_loop(0, chunks + 8 * LAG, tick, 0)

    def drain(j, carry):
        for color in range(2):
            for s in range(4):
                for k, m, far, device in members(orders[color][s]):
                    rs_copy(color, s, j, k, m, far, device).wait_send()
                    if cut[color][s]:
                        ag_copy(color, s, j, k, m, far, device).wait_send()
        return carry

    lax.fori_loop(0, chunks, drain, 0)
    for s in range(4):
        for k, m, far, device in members(orders[0][s]):
            cnt_copy(s, k, m, far, device).wait_send()


def summed_moments(n_gx, n_gy, roi_counts, anchor_counts, mask_g, rpn_g, mask_mo, rpn_mo):
    chunks, chunk, chans = mask_g.shape
    sizes = ((2, n_gx // 2, 2, n_gy // 2), (2, 2, n_gx // 2, n_gy // 2))
    smem, vmem = pl.BlockSpec(memory_space=pltpu.SMEM), pl.BlockSpec(memory_space=pltpu.VMEM)
    hbm = pl.BlockSpec(memory_space=pl.ANY)
    widest = max(max(s) for s in sizes) - 1
    landing, sems = [], []
    for color in range(2):
        b = chunk
        for size in sizes[color]:
            b = b // size if splits(b, size) else b
            landing.append(pltpu.VMEM((chunks, max(size - 1, 1), b, chans), jnp.float32))
            sems.append(pltpu.SemaphoreType.DMA((chunks, max(size - 1, 1))))
    piece = b
    small = [pltpu.SemaphoreType.DMA((max(size - 1, 1),)) for size in sizes[0]]
    out = jax.ShapeDtypeStruct(mask_g.shape, jnp.float32)
    return pl.pallas_call(
        functools.partial(sum_kernel, n_gx, n_gy),
        out_shape=(out, out),
        in_specs=[smem, smem, vmem, vmem, hbm, hbm],
        out_specs=(vmem, vmem),
        scratch_shapes=[
            pltpu.VMEM((2, chunks, chunk, chans), jnp.float32),
            pltpu.VMEM((2, chunks, piece, chans), jnp.float32),
            pltpu.SemaphoreType.DMA((2, chunks)),
            pltpu.VMEM((5, 16, 128), jnp.float32),
            pltpu.VMEM((4, widest, 16, 128), jnp.float32),
        ]
        + landing
        + small
        + small
        + sems * 4,
        compiler_params=pltpu.CompilerParams(
            collective_id=0, has_side_effects=True, vmem_limit_bytes=40 * 2**20
        ),
        name="sum_and_share",
    )(roi_counts, anchor_counts, mask_g, rpn_g, mask_mo, rpn_mo)


def on_device(
    n_gx,
    n_gy,
    mask_feats,
    mask_cot,
    roi_counts,
    rpn_feats,
    rpn_cot,
    anchor_counts,
    mask_weight,
    rpn_weight,
    mask_moment,
    rpn_moment,
):
    mask_g, rpn_g = local_grads(roi_counts, mask_feats, mask_cot, rpn_feats, rpn_cot)
    new_mask, new_rpn = summed_moments(
        n_gx,
        n_gy,
        roi_counts,
        anchor_counts,
        mask_g,
        rpn_g,
        mask_moment.reshape(mask_g.shape),
        rpn_moment.reshape(rpn_g.shape),
    )
    new_mask, new_rpn = new_mask.reshape(mask_moment.shape), new_rpn.reshape(rpn_moment.shape)
    return (mask_weight - 0.02 * new_mask, rpn_weight - 0.02 * new_rpn, new_mask, new_rpn)


def solution(mesh):
    split = P(("gx", "gy"))
    placed = (split,) * 6 + (P(),) * 4
    return jax.shard_map(
        functools.partial(on_device, mesh.shape["gx"], mesh.shape["gy"]),
        mesh=mesh,
        in_specs=placed,
        out_specs=(P(), P(), P(), P()),
        check_vma=False,
    )
```

```python
import functools

import jax
import jax.numpy as jnp
from jax import lax
from jax.experimental import pallas as pl
from jax.experimental.pallas import tpu as pltpu
from jax.sharding import PartitionSpec as P

MESH = pl.DeviceIdType.MESH
TAPS = 9
LAGS = (1, 2, 2, 2, 2, 2, 2, 1)
DUE = tuple(sum(LAGS[: s + 1]) for s in range(8))


def lay_out(x, y, xt, ycat, width, step, count):
    images, depth, chans = x.shape
    lanes = 128
    part = width * max(256 // width, 1)
    while depth % part:
        part -= width
    row = lax.broadcasted_iota(jnp.int32, (part, chans), 0)
    col = lax.rem(row, width)
    for n in range(images):
        for b in range(3):
            ycat[b, n, pl.ds(0, width), :] = jnp.zeros((width, chans), jnp.bfloat16)
            tail = ycat.shape[2] - width - depth
            ycat[b, n, pl.ds(width + depth, tail), :] = jnp.zeros((tail, chans), jnp.bfloat16)
        live = None if count is None else lax.rem(row, step) < count[n]

        def turn(k, carry, n=n):
            at = pl.ds(pl.multiple_of(k * lanes, lanes), lanes)
            xt[n, :, at] = x[n, at, :].T
            return carry

        lax.fori_loop(0, depth // lanes, turn, 0)
        rest = depth % lanes
        if rest:
            last = x[n, pl.ds(depth - rest, rest), :]
            fill = jnp.zeros((lanes - rest, chans), last.dtype)
            xt[n, :, pl.ds(depth - rest, lanes)] = jnp.concatenate([last, fill], axis=0).T

        def move(k, carry, n=n, live=live):
            v = y[n, pl.ds(pl.multiple_of(k * part, 16), part), :].astype(jnp.float32)
            if live is not None:
                v = jnp.where(live, v, 0.0)
            down = jnp.where(col >= width - step, 0.0, pltpu.roll(v, part - step, 0))
            up = jnp.where(col < step, 0.0, pltpu.roll(v, step, 0))
            at = pl.ds(pl.multiple_of(width + k * part, 16), part)
            ycat[0, n, at, :] = down.astype(jnp.bfloat16)
            ycat[1, n, at, :] = v.astype(jnp.bfloat16)
            ycat[2, n, at, :] = up.astype(jnp.bfloat16)
            return carry

        lax.fori_loop(0, depth // part, move, 0)


def one_tap(j, xt, ycat, grad, width):
    images, _, depth = xt.shape
    a, b = lax.div(j, 3), lax.rem(j, 3)
    at = pl.ds(pl.multiple_of((2 - a) * width, 16), depth)
    total = None
    for n in range(images):
        term = jnp.dot(xt[n], ycat[b, n, at, :], preferred_element_type=jnp.float32)
        total = term if total is None else total + term
    grad[j] = total


def splits(rows, size):
    return rows % (8 * size) == 0


def groups_here(n_gx, n_gy):
    gx, gy = lax.axis_index("gx"), lax.axis_index("gy")
    core, x = lax.rem(gx, 2), lax.div(gx, 2)
    y, z = lax.rem(gy, 2), lax.div(gy, 2)
    core_group = (2, core, lambda m: (x * 2 + m, gy))
    x_group = (n_gx // 2, x, lambda m: (m * 2 + core, gy))
    y_group = (2, y, lambda m: (gx, z * 2 + m))
    z_group = (n_gy // 2, z, lambda m: (gx, m * 2 + y))
    return core_group, x_group, y_group, z_group


def members(group):
    size, own, device = group
    return [
        (k, lax.rem(own + 1 + k, size), size - 2 - k, device) for k in range(size - 1)
    ]


def sum_kernel(n_gx, n_gy, widths, steps, *refs):
    roi, anchor = refs[:2]
    given, moments, outs = refs[2:6], refs[6:8], refs[8:10]
    mine, mine_sem, cnt, cnt_in = refs[10:14]
    xts, ycats, grads = refs[14:16], refs[16:18], refs[18:20]
    refs = refs[7:]
    landing = (refs[13:17], refs[17:21])
    cnt_sems = refs[21:25]
    cnt_send = refs[25:29]
    rs_recv = (refs[29:33], refs[33:37])
    rs_send = (refs[37:41], refs[41:45])
    ag_recv = (refs[45:49], refs[49:53])
    ag_send = (refs[53:57], refs[57:61])
    core_g, x_g, y_g, z_g = groups_here(n_gx, n_gy)
    orders = ((core_g, x_g, y_g, z_g), (core_g, y_g, x_g, z_g))
    chunks, chunk = grads[0].shape[:2]

    blocks, offs = [], []
    cut = ([], [])
    for color in range(2):
        b, o, bs, os = chunk, 0, [], [0]
        rest = chunk
        for size, _, _ in orders[color]:
            cut[color].append(splits(rest, size))
            rest = rest // size if cut[color][-1] else rest
        for size, own, _ in orders[color]:
            if splits(b, size):
                b = b // size
                o = o + own * b
            bs.append(b)
            os.append(o)
        blocks.append(bs)
        offs.append(os)
    piece = blocks[0][3]

    barrier = pltpu.get_barrier_semaphore()
    total = 0
    for g in orders[0]:
        for _, m, _, device in members(g):
            pl.semaphore_signal(barrier, inc=1, device_id=device(m), device_id_type=MESH)
            total += 1

    def own_rows(color, j):
        return pltpu.make_async_copy(
            moments[color].at[j, pl.ds(pl.multiple_of(offs[color][4], 8), piece), :],
            mine.at[color, j],
            mine_sem.at[color, j],
        )

    def start_moments(j, carry):
        own_rows(0, j).start()
        own_rows(1, j).start()
        return carry

    lax.fori_loop(0, chunks, start_moments, 0)
    half = cnt.shape[1] // 2
    lanes = cnt.shape[2]
    for which, ref in ((0, roi), (1, anchor)):
        s = ref[0]
        for i in range(1, ref.shape[0]):
            s = s + ref[i]
        cnt[0, which * half : (which + 1) * half, :] = jnp.full(
            (half, lanes), s.astype(jnp.float32), jnp.float32
        )
    for color, count in ((0, roi), (1, None)):
        lay_out(
            given[2 * color],
            given[2 * color + 1],
            xts[color],
            ycats[color],
            widths[color],
            steps[color],
            count,
        )
    pl.semaphore_wait(barrier, total)

    def cnt_copy(s, k, m, far, device):
        return pltpu.make_async_remote_copy(
            src_ref=cnt.at[s],
            dst_ref=cnt_in.at[s, far],
            send_sem=cnt_send[s].at[k],
            recv_sem=cnt_sems[s].at[far],
            device_id=device(m),
            device_id_type=MESH,
        )

    def cnt_arrival(s, k, m, device):
        return pltpu.make_async_remote_copy(
            src_ref=cnt.at[s],
            dst_ref=cnt_in.at[s, k],
            send_sem=cnt_send[s].at[k],
            recv_sem=cnt_sems[s].at[k],
            device_id=device(m),
            device_id_type=MESH,
        )

    def cnt_start(s):
        for k, m, far, device in members(orders[0][s]):
            cnt_copy(s, k, m, far, device).start()

    def cnt_finish(s):
        value = cnt[s]
        for k, m, far, device in members(orders[0][s]):
            cnt_arrival(s, k, m, device).wait_recv()
            value = value + cnt_in[s, k]
        cnt[s + 1] = value

    def rs_copy(color, s, j, k, m, far, device):
        b = blocks[color][s]
        start = offs[color][s] + (m * b if cut[color][s] else 0)
        rows = pl.ds(pl.multiple_of(start, 8), b)
        source = grads[color].at[j, rows, :]
        return pltpu.make_async_remote_copy(
            src_ref=source,
            dst_ref=landing[color][s].at[j, far],
            send_sem=rs_send[color][s].at[j, k],
            recv_sem=rs_recv[color][s].at[j, far],
            device_id=device(m),
            device_id_type=MESH,
        )

    def rs_arrival(color, s, j, k, m, device):
        b = blocks[color][s]
        start = offs[color][s] + (m * b if cut[color][s] else 0)
        rows = pl.ds(pl.multiple_of(start, 8), b)
        source = grads[color].at[j, rows, :]
        return pltpu.make_async_remote_copy(
            src_ref=source,
            dst_ref=landing[color][s].at[j, k],
            send_sem=rs_send[color][s].at[j, k],
            recv_sem=rs_recv[color][s].at[j, k],
            device_id=device(m),
            device_id_type=MESH,
        )

    def rs_start(color, s, j):
        for k, m, far, device in members(orders[color][s]):
            rs_copy(color, s, j, k, m, far, device).start()

    def rs_sum(color, s, j):
        b = blocks[color][s]
        rows = pl.ds(pl.multiple_of(offs[color][s + 1], 8), b)
        value = grads[color][j, rows, :]
        for k, m, _, device in members(orders[color][s]):
            rs_arrival(color, s, j, k, m, device).wait_recv()
            if cut[color][s]:
                value = value + landing[color][s][j, k]
        if not cut[color][s]:
            size, own, _ = orders[color][s]
            terms = []
            for m in range(size):
                slot = lax.rem(m - own - 1 + 2 * size, size)
                slot = jnp.minimum(slot, max(size - 2, 0))
                here = own == m
                terms.append(jnp.where(here, value, landing[color][s][j, slot]))
            value = functools.reduce(jnp.add, terms) if size > 1 else value
        if s < 3:
            grads[color][j, rows, :] = value
        else:
            own_rows(color, j).wait()
            count = cnt[4, color * half : (color + 1) * half, :][0:1, :]
            count = jnp.concatenate([count] * (value.shape[1] // lanes), axis=1)
            outs[color][j, rows, :] = 0.9 * mine[color, j] + value / count

    def ag_copy(color, s, j, k, m, far, device):
        b = blocks[color][s]
        rows = pl.ds(pl.multiple_of(offs[color][s + 1], 8), b)
        return pltpu.make_async_remote_copy(
            src_ref=outs[color].at[j, rows, :],
            dst_ref=outs[color].at[j, rows, :],
            send_sem=ag_send[color][s].at[j, k],
            recv_sem=ag_recv[color][s].at[j, far],
            device_id=device(m),
            device_id_type=MESH,
        )

    def ag_arrival(color, s, j, k, m, device):
        b = blocks[color][s]
        rows = pl.ds(pl.multiple_of(offs[color][s] + m * b, 8), b)
        return pltpu.make_async_remote_copy(
            src_ref=outs[color].at[j, rows, :],
            dst_ref=outs[color].at[j, rows, :],
            send_sem=ag_send[color][s].at[j, k],
            recv_sem=ag_recv[color][s].at[j, k],
            device_id=device(m),
            device_id_type=MESH,
        )

    def ag_start(color, s, j):
        if not cut[color][s]:
            return
        for k, m, far, device in members(orders[color][s]):
            ag_copy(color, s, j, k, m, far, device).start()

    def ag_wait(color, s, j):
        if not cut[color][s]:
            return
        for k, m, _, device in members(orders[color][s]):
            ag_arrival(color, s, j, k, m, device).wait_recv()

    def at_stage(t, lag, work):
        j = t - lag

        @pl.when((j >= 0) & (j < chunks))
        def _():
            work(j)

    def tick(t, carry):
        def first(j):
            for color in range(2):
                rs_start(color, 0, j)

        at_stage(t, 1, first)

        for s in range(4):

            @pl.when(t == DUE[s])
            def _(s=s):
                cnt_finish(s)
                if s < 3:
                    cnt_start(s + 1)

        for s in (3, 2, 1, 0):

            def gather(j, s=s):
                for color in range(2):
                    ag_wait(color, s, j)
                    if s > 0:
                        ag_start(color, s - 1, j)

            at_stage(t, 1 + DUE[7 - s], gather)
        for s in range(4):

            def reduce(j, s=s):
                for color in range(2):
                    rs_sum(color, s, j)
                for color in range(2):
                    if s < 3:
                        rs_start(color, s + 1, j)
                    else:
                        ag_start(color, 3, j)

            at_stage(t, 1 + DUE[s], reduce)

        def taps(j):
            for color in range(2):
                one_tap(j, xts[color], ycats[color], grads[color], widths[color])

        at_stage(t, 0, taps)
        return carry

    cnt_start(0)
    lax.fori_loop(0, 1 + chunks + DUE[-1], tick, 0)

    def drain(j, carry):
        for color in range(2):
            for s in range(4):
                for k, m, far, device in members(orders[color][s]):
                    rs_copy(color, s, j, k, m, far, device).wait_send()
                    if cut[color][s]:
                        ag_copy(color, s, j, k, m, far, device).wait_send()
        return carry

    lax.fori_loop(0, chunks, drain, 0)
    for s in range(4):
        for k, m, far, device in members(orders[0][s]):
            cnt_copy(s, k, m, far, device).wait_send()


def summed_moments(n_gx, n_gy, widths, steps, roi_counts, anchor_counts, fields, moments):
    chunks, chunk, chans = moments[0].shape
    sizes = ((2, n_gx // 2, 2, n_gy // 2), (2, 2, n_gx // 2, n_gy // 2))
    smem, vmem = pl.BlockSpec(memory_space=pltpu.SMEM), pl.BlockSpec(memory_space=pltpu.VMEM)
    hbm = pl.BlockSpec(memory_space=pl.ANY)
    widest = max(max(s) for s in sizes) - 1
    landing, sems = [], []
    for color in range(2):
        b = chunk
        for size in sizes[color]:
            b = b // size if splits(b, size) else b
            landing.append(pltpu.VMEM((chunks, max(size - 1, 1), b, chans), jnp.float32))
            sems.append(pltpu.SemaphoreType.DMA((chunks, max(size - 1, 1))))
    piece = b
    small = [pltpu.SemaphoreType.DMA((max(size - 1, 1),)) for size in sizes[0]]
    out = jax.ShapeDtypeStruct(moments[0].shape, jnp.float32)
    xts, ycats = [], []
    for color in range(2):
        images, depth, _ = fields[2 * color].shape
        padded = -(-depth // 128) * 128
        xts.append(pltpu.VMEM((images, chans, padded), jnp.bfloat16))
        ycats.append(pltpu.VMEM((3, images, padded + 2 * widths[color], chans), jnp.bfloat16))
    return pl.pallas_call(
        functools.partial(sum_kernel, n_gx, n_gy, widths, steps),
        out_shape=(out, out),
        in_specs=[smem, smem] + [vmem] * 4 + [hbm] * 2,
        out_specs=(vmem, vmem),
        scratch_shapes=[
            pltpu.VMEM((2, chunks, piece, chans), jnp.float32),
            pltpu.SemaphoreType.DMA((2, chunks)),
            pltpu.VMEM((5, 16, 128), jnp.float32),
            pltpu.VMEM((4, widest, 16, 128), jnp.float32),
        ]
        + xts
        + ycats
        + [pltpu.VMEM(moments[0].shape, jnp.float32)] * 2
        + landing
        + small
        + small
        + sems * 4,
        compiler_params=pltpu.CompilerParams(
            collective_id=0, has_side_effects=True, vmem_limit_bytes=43 * 2**20
        ),
        name="grads_and_sum",
    )(roi_counts, anchor_counts, *fields, *moments)


def finish_kernel(w0, w1, m0, m1, nw0, nw1, nm0, nm1, s0, s1, m_sem, w_sem):
    copies = []
    for i, (m, out) in enumerate(((m0, nm0), (m1, nm1))):
        copies.append(pltpu.make_async_copy(m, out, m_sem.at[i]))
    for copy in copies:
        copy.start()
    rows = w0.shape[0]
    parts = w_sem.shape[1]
    step = rows // parts
    for i, (w, m, s, out) in enumerate(((w0, m0, s0, nw0), (w1, m1, s1, nw1))):
        for k in range(parts):
            at = pl.ds(k * step, step)
            s[at, :] = w[at, :] - 0.02 * m[at, :]
            copy = pltpu.make_async_copy(s.at[at, :], out.at[at, :], w_sem.at[i, k])
            copy.start()
            copies.append(copy)
    for copy in copies:
        copy.wait()


def finish(weights, moments):
    out = jax.ShapeDtypeStruct(weights[0].shape, jnp.float32)
    vmem, hbm = pl.BlockSpec(memory_space=pltpu.VMEM), pl.BlockSpec(memory_space=pl.ANY)
    return pl.pallas_call(
        finish_kernel,
        out_shape=(out,) * 4,
        in_specs=[vmem] * 4,
        out_specs=(hbm,) * 4,
        scratch_shapes=[
            pltpu.VMEM(weights[0].shape, jnp.float32),
            pltpu.VMEM(weights[0].shape, jnp.float32),
            pltpu.SemaphoreType.DMA((2,)),
            pltpu.SemaphoreType.DMA((2, 3)),
        ],
        compiler_params=pltpu.CompilerParams(vmem_limit_bytes=16 * 2**20),
        name="finish",
    )(*weights, *moments)


def on_device(
    n_gx,
    n_gy,
    mask_feats,
    mask_cot,
    roi_counts,
    rpn_feats,
    rpn_cot,
    anchor_counts,
    mask_weight,
    rpn_weight,
    mask_moment,
    rpn_moment,
):
    images, slots, side, _, chans = mask_feats.shape
    grid_cols = rpn_feats.shape[2]
    fields = [v.transpose(0, 2, 3, 1, 4).reshape(images, -1, chans) for v in (mask_feats, mask_cot)]
    fields += [v.reshape(images, -1, chans) for v in (rpn_feats, rpn_cot)]
    taps = (TAPS, mask_moment.shape[0] // TAPS, chans)
    moments = summed_moments(
        n_gx,
        n_gy,
        (side * slots, grid_cols),
        (slots, 1),
        roi_counts,
        anchor_counts,
        fields,
        (mask_moment.reshape(taps), rpn_moment.reshape(taps)),
    )
    moments = [m.reshape(mask_moment.shape) for m in moments]
    return tuple(finish((mask_weight, rpn_weight), moments))


def solution(mesh):
    split = P(("gx", "gy"))
    placed = (split,) * 6 + (P(),) * 4
    return jax.shard_map(
        functools.partial(on_device, mesh.shape["gx"], mesh.shape["gy"]),
        mesh=mesh,
        in_specs=placed,
        out_specs=(P(), P(), P(), P()),
        check_vma=False,
    )
```
